512 devices in a mesh: groups: 2 (over y), expert: 128 (over z, x), dp: 2 (over core).
Axes of the slice: x: 8, y: 2, z: 16, core: 2. Of those that a mesh axis runs over, the one named last changes fastest.
The devices are a block of a 8x8x16 slice.
Arguments:
- tokens: bfloat16 [32768, 2560], P(('groups', 'expert', 'dp')), parts along dimension 0, may hold values from -6 to 6
- group_ids: int32 [32768, 3], P(('groups', 'expert', 'dp')), parts along dimension 0, may hold values from 0 to 31, as said below
- expert_ids: int32 [32768, 6], P(('groups', 'expert', 'dp')), parts along dimension 0, may hold values from 0 to 95, as said below
- gate_weights: bfloat16 [32768, 6], P(('groups', 'expert', 'dp')), parts along dimension 0, may hold values from 0.019897461 to 0.59765625
- gate_proj: bfloat16 [128, 2560, 576], P('expert', 'dp'), may hold values from -0.125 to 0.125
- up_proj: bfloat16 [128, 2560, 576], P('expert', 'dp'), may hold values from -0.125 to 0.125
- down_proj: bfloat16 [128, 2560, 576], P('expert', 'dp'), may hold values from -0.21875 to 0.21875
Outputs:
- moe_out: bfloat16 [32768, 2560], P(('groups', 'expert', 'dp')), parts along dimension 0
The draws below stay inside these ranges and needn't reach their ends.
There are 2 independent parts, one for each index of `groups`. The reference program is written for one: setup_inputs(seed, part) draws one part's arguments, and reference() takes and returns one part's arrays. A program takes and returns all parts, laid end to end along the dimension named above; an argument that names none is the same for every part. Nothing has to cross between parts.
Inputs may be any that keep to these rules, and one draw needn't show every extreme that they name: `group_ids`: each row holds 3 distinct expert groups. `expert_ids`: each row holds 6 distinct experts, each of them in one of the row's groups; expert e belongs to group e // 3.
All inputs are finite; a program needn't handle non-finite values.
Results may differ from the reference program's by a relative error of at most 0.0078.
Values may be sent and summed in bfloat16 or wider, within the bound.
No kernel may reach another device: no remote copies, remote signals or barrier semaphores. Data moves between devices by JAX's collectives and lax.ppermute only.
A program may use at most 128 MiB of HBM per device.

```python
import math
import jax
import jax.numpy as jnp
from jax import lax

D = 2560
HID = 768
GROUP_EXP = 3
SPAN = 4
TOPK = 6
TOK_DEV = 64
CAP = 8
GROUPS = 32
HSLICE = 192
ROUTE_GROUPS = 3
TOKENS = 16384
N_EXPERT = 128


def route_draw(key):
    base = jax.random.fold_in(key, 7)
    key_bias, key_noise, key_pick = jax.random.split(base, 3)
    bias = jax.random.randint(key_bias, (GROUPS,), 0, 400)
    noise = jax.random.randint(key_noise, (TOKENS, GROUPS), 0, 1000)
    scores = (bias[None, :] + noise) * GROUPS + jnp.arange(GROUPS, dtype=jnp.int32)[None, :]
    unused, chosen = lax.top_k(scores, ROUTE_GROUPS)
    chosen = chosen.astype(jnp.int32)
    width_cand = ROUTE_GROUPS * GROUP_EXP
    candidates = (chosen[:, :, None] * GROUP_EXP + jnp.arange(GROUP_EXP, dtype=jnp.int32)).reshape(TOKENS, width_cand)
    pick_scores = jax.random.randint(key_pick, (TOKENS, width_cand), 0, 1000) * width_cand + jnp.arange(width_cand, dtype=jnp.int32)[None, :]
    unused_two, picked = lax.top_k(pick_scores, TOPK)
    experts = jnp.take_along_axis(candidates, picked.astype(jnp.int32), axis=1)
    return (chosen, experts.astype(jnp.int32))


def draw_group_ids(key, part):
    return route_draw(key)[0]


def draw_expert_ids(key, part):
    return route_draw(key)[1]


def levels(key, dims, cuts, least, high):
    level = 1.0
    for dim, parts in cuts:
        steps = jax.random.uniform(jax.random.fold_in(jax.random.fold_in(key, 6), dim), (parts,), jnp.float32, least / len(cuts), high / len(cuts))
        level = level * jnp.repeat(jnp.exp(steps), dims[dim] // parts).reshape((-1,) + (1,) * (len(dims) - 1 - dim))
    return level


def normal_values(own_key, dims, deviation, reach, cuts=(), kind=jnp.bfloat16):
    values = deviation * jax.random.normal(own_key, dims, jnp.float32)
    if cuts:
        values = values * levels(own_key, dims, cuts, -0.22, 0.18)
    return jnp.clip(values, -reach, reach).astype(kind)


def setup_inputs(seed: int = 0, part: int = 0) -> dict:
    streams_of = jax.random.split(jax.random.key(seed), 8)
    part_splits = jax.random.split(jax.random.fold_in(streams_of[7], part), 8)
    return {
        "tokens": normal_values(part_splits[0], (TOKENS, D), 1.0, 6.0, ((0, 256),)),
        "group_ids": draw_group_ids(jax.random.fold_in(jax.random.fold_in(streams_of[7], part), 71), part),
        "expert_ids": draw_expert_ids(jax.random.fold_in(jax.random.fold_in(streams_of[7], part), 71), part),
        "gate_weights": jnp.clip(jnp.exp(math.log(0.59765625) - 3.4024236 * jax.random.uniform(part_splits[3], (TOKENS, TOPK), jnp.float32) ** levels(part_splits[3], (TOKENS, TOPK), ((0, 256),), -0.2, 0.2)), 0.019897461, 0.59765625).astype(jnp.bfloat16),
        "gate_proj": normal_values(streams_of[4], (N_EXPERT, D, GROUP_EXP * HSLICE), D ** -0.5, 0.125, ((0, 128), (1, 2))),
        "up_proj": normal_values(streams_of[5], (N_EXPERT, D, GROUP_EXP * HSLICE), D ** -0.5, 0.125, ((0, 128), (1, 2))),
        "down_proj": normal_values(streams_of[6], (N_EXPERT, D, GROUP_EXP * HSLICE), HID ** -0.5, 0.21875, ((0, 128), (1, 2))),
    }


def reference(tokens, group_ids, expert_ids, gate_weights, gate_proj, up_proj, down_proj):
    shards = TOKENS // TOK_DEV
    inputs = tokens.astype(jnp.float32).reshape(shards, TOK_DEV, D)
    chosen = group_ids.reshape(shards, TOK_DEV, ROUTE_GROUPS)
    experts = expert_ids.reshape(shards, TOK_DEV, TOPK)
    weights = gate_weights.astype(jnp.float32).reshape(shards, TOK_DEV, TOPK)
    group_iota = jnp.arange(GROUPS, dtype=jnp.int32)
    member = jnp.sum((chosen[..., None] == group_iota).astype(jnp.int32), axis=2)
    rank = jnp.cumsum(member, axis=1) - member
    kept = member * (rank < CAP).astype(jnp.int32)
    slot_iota = jnp.arange(CAP, dtype=jnp.int32)
    width_cols = GROUP_EXP * HSLICE

    def one_group(total, group):
        select = (kept[:, :, group][..., None] * (rank[:, :, group][..., None] == slot_iota).astype(jnp.int32)).astype(jnp.float32)
        local_experts = group * GROUP_EXP + jnp.arange(GROUP_EXP, dtype=jnp.int32)
        factor = jnp.sum(weights[..., None] * (experts[..., None] == local_experts).astype(jnp.float32), axis=2)
        rows = jnp.einsum('stc,std->scd', select, inputs).reshape(shards * CAP, D)
        row_factor = jnp.einsum('stc,stk->sck', select, factor).reshape(shards * CAP, GROUP_EXP)
        start = (group * SPAN).astype(jnp.int32)
        w_gate = lax.dynamic_slice_in_dim(gate_proj, start, SPAN, 0).astype(jnp.float32)
        w_up = lax.dynamic_slice_in_dim(up_proj, start, SPAN, 0).astype(jnp.float32)
        w_down = lax.dynamic_slice_in_dim(down_proj, start, SPAN, 0).astype(jnp.float32)
        gate_h = jnp.einsum('rd,pdc->rpc', rows, w_gate)
        up_h = jnp.einsum('rd,pdc->rpc', rows, w_up)
        hidden = (jax.nn.silu(gate_h) * up_h).reshape(shards * CAP, SPAN, GROUP_EXP, HSLICE)
        hidden = hidden * row_factor[:, None, :, None]
        hidden = lax.optimization_barrier(hidden.astype(jnp.bfloat16)).astype(jnp.float32)
        hidden = hidden.reshape(shards * CAP, SPAN, width_cols)
        result = jnp.einsum('rpc,pdc->rd', hidden, w_down)
        result = lax.optimization_barrier(result.astype(jnp.bfloat16)).astype(jnp.float32)
        result = result.reshape(shards, CAP, D)
        return total + jnp.einsum('stc,scd->std', select, result), None

    start_total = jnp.zeros((shards, TOK_DEV, D), jnp.float32)
    total, unused = lax.scan(one_group, start_total, jnp.arange(GROUPS, dtype=jnp.int32))
    return total.reshape(TOKENS, D).astype(jnp.bfloat16)
```

```python
import jax
import jax.numpy as jnp
from jax import lax
from jax.sharding import PartitionSpec as P

GROUP_EXP = 3
SPAN = 4
CAP = 8
COLS = 2 * SPAN
LANES = 128
CHUNKS = 1


def hop(col, k):
    step = (0, -1, 2, -3)[k]
    return (col + step if col % 2 == 0 else col - step) % COLS


def back(col, k):
    return next(c for c in range(COLS) if hop(c, k) == col)


def along_x(value, move):
    count = lax.axis_size("expert")
    route = [(e, e - e % COLS + move(e % COLS)) for e in range(count)]
    return lax.ppermute(value, "expert", route)


def over_z(value):
    count = lax.axis_size("expert")
    lines = [list(range(c, count, COLS)) for c in range(COLS)]
    return lax.all_to_all(value, "expert", 0, 0, axis_index_groups=lines, tiled=True)


def pair_swap(value):
    return along_x(value, lambda c: c ^ 1)


def core_swap(value):
    return lax.ppermute(value, "dp", [(0, 1), (1, 0)])


def own_first(value):
    half = value.shape[-1] // 2
    lower, upper = value[..., :half], value[..., half:]
    first = lax.axis_index("dp") == 0
    return jnp.concatenate(
        [jnp.where(first, lower, upper), jnp.where(first, upper, lower)], axis=-1
    )


def contract(a, b):
    return lax.dot_general(a, b, (((1,), (1,)), ((), ())), preferred_element_type=jnp.float32)


def body(tokens, group_ids, expert_ids, gate_weights, gate_proj, up_proj, down_proj):
    n_tok, width = tokens.shape
    half = width // 2
    n_expert = lax.axis_size("expert")
    n_groups = n_expert // SPAN
    n_rows = n_expert // COLS
    part = CAP // CHUNKS
    index = lax.axis_index("expert")
    col = index % COLS
    group = index // SPAN

    own = [jnp.swapaxes(w[0], 0, 1) for w in (gate_proj, up_proj, down_proj)]
    pair = [pair_swap(w) for w in own]
    own_far = [core_swap(w) for w in own]
    pair_far = [core_swap(w) for w in pair]

    group_iota = jnp.arange(n_groups, dtype=jnp.int32)
    member = jnp.sum((group_ids[:, :, None] == group_iota).astype(jnp.int32), axis=1)
    rank = jnp.cumsum(member, axis=0) - member
    kept = member * (rank < CAP).astype(jnp.int32)
    slot_iota = jnp.arange(CAP, dtype=jnp.int32)
    select = (kept[:, :, None] * (rank[:, :, None] == slot_iota).astype(jnp.int32)).astype(
        jnp.bfloat16
    )
    table_iota = jnp.arange(-(-n_groups * GROUP_EXP // LANES) * LANES, dtype=jnp.int32)
    matches = expert_ids[:, :, None] == table_iota
    table = jnp.sum(
        jnp.where(matches, gate_weights[:, :, None].astype(jnp.float32), 0.0), axis=1
    ).astype(jnp.bfloat16)
    sent = jnp.concatenate([own_first(tokens), table], axis=1)

    hidden_cols = own[0].shape[0]
    spread_to = GROUP_EXP * group + jnp.arange(hidden_cols, dtype=jnp.int32) // (
        hidden_cols // GROUP_EXP
    )
    spread = (table_iota[:, None] == spread_to[None, :]).astype(jnp.bfloat16)
    halves = [
        jnp.asarray([hop(c, k) // SPAN for c in range(COLS)], jnp.int32)[col] for k in range(4)
    ]

    outs = []
    for i in range(CHUNKS):
        pick = select[:, :, i * part : (i + 1) * part]
        rows = jnp.einsum("tgc,td->gcd", pick, sent, preferred_element_type=jnp.float32)
        rows = rows.astype(jnp.bfloat16).reshape(n_rows, 2 * part, sent.shape[1])
        got = over_z(rows).reshape(n_rows, 2, part, sent.shape[1])
        units = []
        for k in range(4):
            unit = lax.dynamic_index_in_dim(got, halves[k], 1, keepdims=False)
            unit = unit.reshape(n_rows * part, sent.shape[1])
            units.append(unit if k == 0 else along_x(unit, lambda c: hop(c, k)))
        x = jnp.concatenate(units, axis=0)
        near, far = x[:, :half], x[:, half:width]
        scale = jnp.dot(x[:, width:], spread, preferred_element_type=jnp.float32)
        hidden = []
        for w, w_far in ((own, own_far), (pair, pair_far)):
            gate_h = contract(near, w[0]) + contract(far, w_far[0])
            up_h = contract(near, w[1]) + contract(far, w_far[1])
            hidden.append((jax.nn.silu(gate_h) * up_h * scale).astype(jnp.bfloat16))
        partial = jnp.concatenate(
            [
                jnp.dot(hidden[0], own[2], preferred_element_type=jnp.float32)
                + jnp.dot(hidden[1], pair[2], preferred_element_type=jnp.float32),
                jnp.dot(hidden[0], own_far[2], preferred_element_type=jnp.float32)
                + jnp.dot(hidden[1], pair_far[2], preferred_element_type=jnp.float32),
            ],
            axis=1,
        ).astype(jnp.bfloat16)
        shares = jnp.split(partial, 4, axis=0)
        shares = [
            share if k == 0 else along_x(share, lambda c: back(c, k))
            for k, share in enumerate(shares)
        ]
        both = [
            sum(
                jnp.where(halves[k] == h, shares[k].astype(jnp.float32), 0.0) for k in range(4)
            ).astype(jnp.bfloat16)
            for h in range(2)
        ]
        both = jnp.stack([b.reshape(n_rows, part, width) for b in both], axis=1)
        returned = over_z(both.reshape(n_rows, 2 * part, width))
        returned = returned.reshape(n_groups, part, width)
        outs.append(
            jnp.einsum("tgc,gcd->td", pick, returned, preferred_element_type=jnp.float32)
        )
    result = outs[0]
    for extra in outs[1:]:
        result = result + extra
    return own_first(result.astype(jnp.bfloat16))


def solution(mesh):
    placed = (
        P(("groups", "expert", "dp"), None),
        P(("groups", "expert", "dp"), None),
        P(("groups", "expert", "dp"), None),
        P(("groups", "expert", "dp"), None),
        P("expert", "dp", None),
        P("expert", "dp", None),
        P("expert", "dp", None),
    )
    return jax.shard_map(
        body,
        mesh=mesh,
        in_specs=placed,
        out_specs=P(("groups", "expert", "dp"), None),
        check_vma=False,
    )
```

```python
import jax
import jax.numpy as jnp
from jax import lax
from jax.sharding import PartitionSpec as P

GROUP_EXP = 3
SPAN = 4
CAP = 8
COLS = 2 * SPAN
LANES = 128
CHUNKS = 2


STEPS = (0, -1, 2, -3)


def hop(col, k):
    return (col + STEPS[k] if col % 2 == 0 else col - STEPS[k]) % COLS


def back(col, k):
    return next(c for c in range(COLS) if hop(c, k) == col)


def along_x(value, move):
    count = lax.axis_size("expert")
    route = [(e, e - e % COLS + move(e % COLS)) for e in range(count)]
    return lax.ppermute(value, "expert", route)


def over_z(value):
    count = lax.axis_size("expert")
    lines = [list(range(c, count, COLS)) for c in range(COLS)]
    return lax.all_to_all(value, "expert", 0, 0, axis_index_groups=lines, tiled=True)


def pair_swap(value):
    return along_x(value, lambda c: c ^ 1)


def core_swap(value):
    return lax.ppermute(value, "dp", [(0, 1), (1, 0)])


def own_first(value):
    half = value.shape[-1] // 2
    lower, upper = value[..., :half], value[..., half:]
    first = lax.axis_index("dp") == 0
    return jnp.concatenate(
        [jnp.where(first, lower, upper), jnp.where(first, upper, lower)], axis=-1
    )


def contract(a, b):
    return lax.dot_general(a, b, (((1,), (1,)), ((), ())), preferred_element_type=jnp.float32)


def experts(x, width, weights, spread):
    half = width // 2
    near, far = x[:, :half], x[:, half:width]
    scale = jnp.dot(x[:, width:], spread, preferred_element_type=jnp.float32)
    hidden = []
    for w, w_far in weights:
        gate_h = contract(near, w[0]) + contract(far, w_far[0])
        up_h = contract(near, w[1]) + contract(far, w_far[1])
        hidden.append((jax.nn.silu(gate_h) * up_h * scale).astype(jnp.bfloat16))
    total = [
        sum(
            jnp.dot(h, w[side][2], preferred_element_type=jnp.float32)
            for h, w in zip(hidden, weights)
        )
        for side in range(2)
    ]
    return jnp.concatenate(total, axis=1).astype(jnp.bfloat16)


def layer(tokens, group_ids, expert_ids, gate_weights, gate_proj, up_proj, down_proj):
    _, width = tokens.shape
    n_expert = lax.axis_size("expert")
    n_groups = n_expert // SPAN
    n_rows = n_expert // COLS
    part = CAP // CHUNKS
    index = lax.axis_index("expert")
    col = index & (COLS - 1)
    group = index // SPAN

    own = [jnp.swapaxes(w[0], 0, 1) for w in (gate_proj, up_proj, down_proj)]
    pair, own_far, pair_far = [], [], []
    for n, w in enumerate(own):
        pair.append(pair_swap(w))
        own_far.append(core_swap(w))
        pair_far.append(core_swap(pair[n]))

    weights = ((own, own_far), (pair, pair_far))

    group_iota = jnp.arange(n_groups, dtype=jnp.int32)
    member = jnp.sum((group_ids[:, :, None] == group_iota).astype(jnp.int32), axis=1)
    rank = jnp.cumsum(member, axis=0) - member
    kept = member * (rank < CAP).astype(jnp.int32)
    slot_iota = jnp.arange(CAP, dtype=jnp.int32)
    select = (kept[:, :, None] * (rank[:, :, None] == slot_iota).astype(jnp.int32)).astype(
        jnp.bfloat16
    )
    table_iota = jnp.arange(-(-n_groups * GROUP_EXP // LANES) * LANES, dtype=jnp.int32)
    matches = expert_ids[:, :, None] == table_iota
    table = jnp.sum(
        jnp.where(matches, gate_weights[:, :, None].astype(jnp.float32), 0.0), axis=1
    ).astype(jnp.bfloat16)
    sent = jnp.concatenate([own_first(tokens), table], axis=1)

    hidden_cols = own[0].shape[0]
    spread_to = GROUP_EXP * group + jnp.arange(hidden_cols, dtype=jnp.int32) // (
        hidden_cols // GROUP_EXP
    )
    spread = (table_iota[:, None] == spread_to[None, :]).astype(jnp.bfloat16)
    sign = 1 - 2 * (col & 1)
    halves = [((col + sign * STEPS[k]) & (COLS - 1)) // SPAN for k in range(4)]

    picks, gots, inputs, partials = [], [], [], []
    for i in range(CHUNKS):
        pick = select[:, :, i * part : (i + 1) * part]
        rows = jnp.einsum("tgc,td->gcd", pick, sent, preferred_element_type=jnp.float32)
        rows = rows.astype(jnp.bfloat16)
        got = over_z(rows)
        picks.append(pick)
        gots.append(got.reshape(n_rows, 2, part, sent.shape[1]))
    for i in range(CHUNKS):
        got = gots[i]
        if i > 0:
            got, _ = lax.optimization_barrier((got, inputs[i - 1][1]))
        units = []
        for k in range(4):
            unit = lax.dynamic_index_in_dim(got, halves[k], 1, keepdims=False)
            units.append(unit.reshape(n_rows * part, sent.shape[1]))
        for k in range(1, 4):
            units[k] = along_x(units[k], lambda c: hop(c, k))
        inputs.append(units)
    for i in range(CHUNKS):
        units = inputs[i]
        if i > 0:
            units, _ = lax.optimization_barrier((units, partials[i - 1]))
        partials.append(experts(jnp.concatenate(units, axis=0), width, weights, spread))
    outs = []
    for i in range(CHUNKS):
        shares = jnp.split(partials[i], 4, axis=0)
        for k in range(1, 4):
            shares[k] = along_x(shares[k], lambda c: back(c, k))
        both = [
            sum(
                jnp.where(halves[k] == h, shares[k].astype(jnp.float32), 0.0) for k in range(4)
            ).astype(jnp.bfloat16)
            for h in range(2)
        ]
        both = jnp.stack([b.reshape(n_rows, part, width) for b in both], axis=1)
        returned = over_z(both.reshape(2 * n_rows, part, width))
        outs.append(
            jnp.einsum("tgc,gcd->td", picks[i], returned, preferred_element_type=jnp.float32)
        )
    result = outs[0]
    for extra in outs[1:]:
        result = result + extra
    return own_first(result.astype(jnp.bfloat16))


def solution(mesh):
    placed = (
        P(("groups", "expert", "dp"), None),
        P(("groups", "expert", "dp"), None),
        P(("groups", "expert", "dp"), None),
        P(("groups", "expert", "dp"), None),
        P("expert", "dp", None),
        P("expert", "dp", None),
        P("expert", "dp", None),
    )
    return jax.shard_map(
        layer,
        mesh=mesh,
        in_specs=placed,
        out_specs=P(("groups", "expert", "dp"), None),
        check_vma=False,
    )
```
